128 devices in a mesh: owner: 8 (over x, core), rows: 16 (over z, y).
Axes of the slice: x: 4, y: 4, z: 4, core: 2. Of those that a mesh axis runs over, the one named last changes fastest.
Arguments:
- master_gate: float32 [64, 2048, 1024], P('owner', 'rows'), may hold values from -0.1875 to 0.1875
- second_gate: bfloat16 [64, 2048, 1024], P('owner', 'rows'), may hold values from -0.0625 to 0.0625
- master_up: float32 [64, 2048, 1024], P('owner', 'rows'), may hold values from -0.1875 to 0.1875
- second_up: bfloat16 [64, 2048, 1024], P('owner', 'rows'), may hold values from -0.0625 to 0.0625
- master_down: float32 [64, 1024, 2048], P('owner', None, 'rows'), may hold values from -0.25 to 0.25
- second_down: bfloat16 [64, 1024, 2048], P('owner', None, 'rows'), may hold values from -0.09375 to 0.09375
- router_weight: float32 [2048, 64], P('rows', 'owner'), may hold values from -0.125 to 0.125
- router_gain: float32 [2048], P('rows'), may hold values from 0.25 to 1.75
Outputs:
- final_gate: bfloat16 [64, 2048, 1024], P('owner', None, 'rows')
- final_up: bfloat16 [64, 2048, 1024], P('owner', None, 'rows')
- final_down: bfloat16 [64, 1024, 2048], P('owner', 'rows')
- scale_gate: float32 [64, 1024], P('owner', 'rows')
- scale_up: float32 [64, 1024], P('owner', 'rows')
- scale_down: float32 [64, 1024], P('owner', 'rows')
- serve_router: bfloat16 [2048, 64], replicated
The draws below stay inside these ranges and needn't reach their ends.
All inputs are finite; a program needn't handle non-finite values.
Results may differ from the reference program's by a relative error of at most 0.001.
Values may be sent and summed in bfloat16 or wider, within the bound.
A program may use at most 128 MiB of HBM per device.

```python
import jax
import jax.numpy as jnp
from jax import lax

EXPERTS = 64
D_MODEL = 2048
D_EXPERT = 1024


def with_spikes(values, stream_key, source, target, parts, factor):
    def block_of(position):
        return (jnp.arange(values.shape[position]) // (values.shape[position] // parts)).reshape((-1,) + (1,) * (values.ndim - 1 - position))

    near = jax.random.permutation(stream_key, parts)[block_of(target)]
    second = (block_of(target) + parts // 2) % parts
    return jnp.where((block_of(source) == near) | (block_of(source) == second), factor * values, values)


def shard_levels(rng, extent, shards, low, high):
    level = 1.0
    for axis_at, parts in shards:
        draws = jax.random.uniform(jax.random.fold_in(jax.random.fold_in(rng, 6), axis_at), (parts,), jnp.float32, low / len(shards), high / len(shards))
        level = level * jnp.repeat(jnp.exp(draws), extent[axis_at] // parts).reshape((-1,) + (1,) * (len(extent) - 1 - axis_at))
    return level


def scatter_about(stream_key, dims, scale, bound, shards=(), dtype=jnp.bfloat16):
    entries = jax.random.normal(stream_key, dims, jnp.float32) * scale
    if len(shards) > 0:
        entries = shard_levels(stream_key, dims, shards, -0.22, 0.18) * entries
    return jnp.clip(entries, min=-bound, max=bound).astype(dtype)


def noise_with(key, shape, spread, most, split, heavy, kind=jnp.bfloat16):
    array = spread * jax.random.normal(key, shape, jnp.float32)
    if split:
        array = array * shard_levels(key, shape, split, -0.22, 0.18)
    return jnp.clip(with_spikes(array, jax.random.fold_in(key, 3), *heavy), -most, most).astype(kind)


def setup_inputs(seed: int = 0) -> dict:
    key_of = jax.random.split(jax.random.key(seed), 9)
    return {
        "master_gate": noise_with(key_of[0], (EXPERTS, D_MODEL, D_EXPERT), D_MODEL ** -0.5, 0.1875, ((0, 8), (1, 16)), (1, 2, 16, 2.0), jnp.float32),
        "second_gate": scatter_about(key_of[1], (EXPERTS, D_MODEL, D_EXPERT), (D_MODEL * 4) ** -0.5, 0.0625, ((0, 8), (1, 16))),
        "master_up": noise_with(key_of[2], (EXPERTS, D_MODEL, D_EXPERT), D_MODEL ** -0.5, 0.1875, ((0, 8), (1, 16)), (1, 2, 16, 2.0), jnp.float32),
        "second_up": scatter_about(key_of[3], (EXPERTS, D_MODEL, D_EXPERT), (D_MODEL * 4) ** -0.5, 0.0625, ((0, 8), (1, 16))),
        "master_down": noise_with(key_of[4], (EXPERTS, D_EXPERT, D_MODEL), D_EXPERT ** -0.5, 0.25, ((0, 8), (2, 16)), (2, 1, 16, 2.0), jnp.float32),
        "second_down": scatter_about(key_of[5], (EXPERTS, D_EXPERT, D_MODEL), (D_EXPERT * 4) ** -0.5, 0.09375, ((0, 8), (2, 16))),
        "router_weight": scatter_about(key_of[6], (D_MODEL, EXPERTS), D_MODEL ** -0.5, 0.125, ((0, 16), (1, 8)), jnp.float32),
        "router_gain": jnp.clip(1.0 + 0.15 * jax.random.normal(key_of[7], (D_MODEL,), jnp.float32), 0.25, 1.75),
    }


def reference(master_gate, second_gate, master_up, second_up, master_down, second_down, router_weight, router_gain):
    merged_gate = master_gate + second_gate.astype(jnp.float32)
    merged_up = master_up + second_up.astype(jnp.float32)
    merged_down = master_down + second_down.astype(jnp.float32)
    scale_gate = jnp.sqrt(lax.optimization_barrier(jnp.sum(merged_gate * merged_gate, axis=1)))
    final_gate = (merged_gate / jnp.expand_dims(scale_gate, 1)).astype(jnp.bfloat16)
    scale_up = jnp.sqrt(lax.optimization_barrier(jnp.sum(merged_up * merged_up, axis=1)))
    final_up = (merged_up / jnp.expand_dims(scale_up, 1)).astype(jnp.bfloat16)
    scale_down = jnp.sqrt(lax.optimization_barrier(jnp.sum(merged_down * merged_down, axis=2)))
    final_down = (merged_down / jnp.expand_dims(scale_down, 2)).astype(jnp.bfloat16)
    serve_router = (router_weight * router_gain[:, None]).astype(jnp.bfloat16)
    return (final_gate, final_up, final_down, scale_gate, scale_up, scale_down, serve_router)
```

```python
import functools

import jax
import jax.numpy as jnp
from jax import lax
from jax.experimental import pallas as pl
from jax.experimental.pallas import tpu as pltpu
from jax.sharding import PartitionSpec as P

F32 = jnp.float32
BF16 = jnp.bfloat16
MESH = pl.DeviceIdType.MESH
Y = 4
LANES = 128


def exchange_kernel(
    rows,
    owners,
    mg, sg, mu, su, md, sd, rw, gain,
    og, ou, od, sc, ro,
    vmg, vsg, vmu, vsu, vmd, vsd, vrw, vgain,
    send, ps, rb, tt,
    in_sem, small_sem, stat_send, stat_recv, tot_send, tot_recv,
    data_send, data_recv, row_send, row_recv, own_send, own_recv,
):
    experts = mg.shape[0]
    width = mg.shape[2]
    blocks = width // LANES
    mine = width // rows
    halves = rows // blocks
    part = experts // halves
    owner = lax.axis_index("owner")
    me = lax.axis_index("rows")
    z, y = me // Y, me % Y
    peers = [((z + k // Y) % (rows // Y)) * Y + (y + k % Y) % Y for k in range(1, rows)]
    others = [(owner + k) % owners for k in range(1, owners)]

    barrier = pltpu.get_barrier_semaphore()
    for p in peers:
        pl.semaphore_signal(barrier, inc=1, device_id={"rows": p}, device_id_type=MESH)
    for p in others:
        pl.semaphore_signal(barrier, inc=1, device_id={"owner": p}, device_id_type=MESH)

    matrices = (
        (mg, sg, vmg, vsg, og, True),
        (mu, su, vmu, vsu, ou, True),
        (md, sd, vmd, vsd, od, False),
    )

    def loads(m, e):
        master, second, vm, vs = matrices[m][:4]
        return (
            pltpu.make_async_copy(master.at[e], vm.at[e], in_sem.at[2 * m, e]),
            pltpu.make_async_copy(second.at[e], vs.at[e], in_sem.at[2 * m + 1, e]),
        )

    for m in range(3):
        @pl.loop(0, experts)
        def _(e):
            for c in loads(m, e):
                c.start()

    small = (
        pltpu.make_async_copy(rw, vrw, small_sem.at[0]),
        pltpu.make_async_copy(gain, vgain, small_sem.at[1]),
    )
    for c in small:
        c.start()

    for m in range(3):
        vm, vs, across = matrices[m][2], matrices[m][3], matrices[m][5]

        @pl.loop(0, experts)
        def _(e):
            for c in loads(m, e):
                c.wait()
            half, at = e // part, m * part + e % part
            if across:
                acc = jnp.zeros((8, width), F32)
                for i in range(0, vm.shape[1], 16):
                    x = vm[e, i : i + 16, :] + vs[e, i : i + 16, :].astype(F32)
                    x = x * x
                    acc = acc + x[:8] + x[8:]
                total = jnp.sum(acc, axis=0, keepdims=True)
                for b in range(blocks):
                    ps[half, b, pl.ds(at, 1), :] = total[:, b * LANES : (b + 1) * LANES]
            else:
                for b in range(blocks):
                    x = vm[e, b * LANES : (b + 1) * LANES, :] + vs[e, b * LANES : (b + 1) * LANES, :].astype(F32)
                    ps[half, b, pl.ds(at, 1), :] = jnp.sum((x * x).T, axis=0, keepdims=True)

    pl.semaphore_wait(barrier, rows - 1 + owners - 1)

    def stat_copy(p):
        return pltpu.make_async_remote_copy(
            src_ref=ps.at[p // blocks, p % blocks], dst_ref=rb.at[me],
            send_sem=stat_send, recv_sem=stat_recv, device_id={"rows": p}, device_id_type=MESH,
        )

    for p in peers:
        stat_copy(p).start()
    rb[me] = ps[me // blocks, me % blocks]

    lanes = pl.ds(pl.multiple_of(me * LANES, LANES), LANES)
    for c in small:
        c.wait()
    ro[owner, :, lanes] = (vrw[...] * vgain[...]).astype(BF16)

    def row_copy(p):
        return pltpu.make_async_remote_copy(
            src_ref=ro.at[owner, :, lanes], dst_ref=ro.at[owner, :, lanes],
            send_sem=row_send, recv_sem=row_recv, device_id={"rows": p}, device_id_type=MESH,
        )

    for p in peers:
        row_copy(p).start()

    others_rb = rb.at[pl.ds(0, rows - 1)]
    pltpu.make_async_copy(others_rb, others_rb, stat_recv).wait()
    total = rb[0]
    for k in range(1, rows):
        total = total + rb[k]
    tt[me // blocks, me % blocks] = total

    def total_copy(p):
        here = tt.at[me // blocks, me % blocks]
        return pltpu.make_async_remote_copy(
            src_ref=here, dst_ref=here,
            send_sem=tot_send, recv_sem=tot_recv, device_id={"rows": p}, device_id_type=MESH,
        )

    for p in peers:
        total_copy(p).start()
    pltpu.make_async_copy(others_rb, others_rb, tot_recv).wait()

    def data_copy(m, e, p):
        return pltpu.make_async_remote_copy(
            src_ref=send.at[m, e, pl.ds(pl.multiple_of(p * mine, mine), mine)],
            dst_ref=matrices[m][4].at[e, :, lanes],
            send_sem=data_send.at[m], recv_sem=data_recv.at[m],
            device_id={"rows": p}, device_id_type=MESH,
        )

    def own_copy(p):
        return pltpu.make_async_remote_copy(
            src_ref=ro.at[owner], dst_ref=ro.at[owner],
            send_sem=own_send, recv_sem=own_recv, device_id={"owner": p}, device_id_type=MESH,
        )

    for m in range(3):
        vm, vs, out, across = matrices[m][2], matrices[m][3], matrices[m][4], matrices[m][5]

        @pl.loop(0, experts)
        def _(e):
            half, at = e // part, m * part + e % part
            for b in range(blocks):
                sl = slice(b * LANES, (b + 1) * LANES)
                inverse = 1.0 / jnp.sqrt(tt[half, b, pl.ds(at, 1), :])
                if across:
                    x = (vm[e, :, sl] + vs[e, :, sl].astype(F32)) * inverse
                    send[m, e, sl, :] = x.T.astype(BF16)
                else:
                    x = vm[e, sl, :] + vs[e, sl, :].astype(F32)
                    send[m, e, sl, :] = (x * jnp.broadcast_to(inverse, (LANES, LANES)).T).astype(BF16)
            for p in peers:
                data_copy(m, e, p).start()
            out[e, :, lanes] = send[m, e, pl.ds(pl.multiple_of(me * mine, mine), mine), :]

        if m == 0:
            arrived = ro.at[owner, :, pl.ds(0, (rows - 1) * LANES)]
            pltpu.make_async_copy(arrived, arrived, row_recv).wait()
            pltpu.make_async_copy(arrived, arrived, row_send).wait()
            for p in others:
                own_copy(p).start()

    for m in range(3):
        for h in range(halves):
            s = jnp.sqrt(tt[h, me // 2, m * part : (m + 1) * part, :])
            s = jnp.where(me % 2 == 1, pltpu.roll(s, LANES - mine, 1), s)
            sc[m, h * part : (h + 1) * part, :] = s[:, :mine]

    pltpu.make_async_copy(others_rb, others_rb, stat_send).wait()
    pltpu.make_async_copy(others_rb, others_rb, tot_send).wait()
    theirs = ro.at[pl.ds(0, owners - 1)]
    pltpu.make_async_copy(theirs, theirs, own_send).wait()
    pltpu.make_async_copy(theirs, theirs, own_recv).wait()
    for m in range(3):
        sent = send.at[m, :, pl.ds(0, (rows - 1) * mine), :]
        pltpu.make_async_copy(sent, sent, data_send.at[m]).wait()
        pltpu.make_async_copy(sent, sent, data_recv.at[m]).wait()


def store_kernel(og, ou, od, sc, ro, fg, fu, fd, a, b, c, fr, sem):
    copies = [
        pltpu.make_async_copy(og, fg, sem.at[0]),
        pltpu.make_async_copy(ou, fu, sem.at[1]),
        pltpu.make_async_copy(od, fd, sem.at[2]),
        pltpu.make_async_copy(ro, fr, sem.at[3]),
        pltpu.make_async_copy(sc.at[0], a, sem.at[4]),
        pltpu.make_async_copy(sc.at[1], b, sem.at[5]),
        pltpu.make_async_copy(sc.at[2], c, sem.at[6]),
    ]
    for copy in copies:
        copy.start()
    for copy in copies:
        copy.wait()


def solution(mesh):
    owners, rows = mesh.shape["owner"], mesh.shape["rows"]

    def body(mg, sg, mu, su, md, sd, rw, gain):
        experts, deep, width = mg.shape
        blocks = width // LANES
        halves = rows // blocks
        units = 3 * experts // halves
        mine = width // rows
        hbm = pl.BlockSpec(memory_space=pltpu.HBM)
        vmem = pl.BlockSpec(memory_space=pltpu.VMEM)
        result = pltpu.VMEM((experts, mine, rows * LANES), BF16)
        args = [mg, sg, mu, su, md, sd, rw.T, gain[None, :]]
        args = [pltpu.with_memory_space_constraint(x, pltpu.HBM) for x in args]
        og, ou, od, sc, ro = pl.pallas_call(
            functools.partial(exchange_kernel, rows, owners),
            out_shape=[
                result, result, result,
                pltpu.VMEM((3, experts, mine), F32),
                pltpu.VMEM((owners, rw.shape[1], rows * LANES), BF16),
            ],
            in_specs=[hbm] * 8,
            out_specs=[vmem] * 5,
            scratch_shapes=[pltpu.VMEM(x.shape, x.dtype) for x in args]
            + [
                pltpu.VMEM((3, experts, width, LANES), BF16),
                pltpu.VMEM((halves, blocks, units, LANES), F32),
                pltpu.VMEM((rows, units, LANES), F32),
                pltpu.VMEM((halves, blocks, units, LANES), F32),
                pltpu.SemaphoreType.DMA((6, experts)),
                pltpu.SemaphoreType.DMA((2,)),
                pltpu.SemaphoreType.DMA,
                pltpu.SemaphoreType.DMA,
                pltpu.SemaphoreType.DMA,
                pltpu.SemaphoreType.DMA,
                pltpu.SemaphoreType.DMA((3,)),
                pltpu.SemaphoreType.DMA((3,)),
                pltpu.SemaphoreType.DMA,
                pltpu.SemaphoreType.DMA,
                pltpu.SemaphoreType.DMA,
                pltpu.SemaphoreType.DMA,
            ],
            compiler_params=pltpu.CompilerParams(
                collective_id=0, has_side_effects=True, vmem_limit_bytes=44 * 1024 * 1024
            ),
            name="exchange",
        )(*args)
        scale = jax.ShapeDtypeStruct((experts, mine), F32)
        whole = jax.ShapeDtypeStruct((experts, mine, rows * LANES), BF16)
        fg, fu, fd, a, b, c, fr = pl.pallas_call(
            store_kernel,
            out_shape=[whole] * 3 + [scale] * 3 + [jax.ShapeDtypeStruct(ro.shape, BF16)],
            in_specs=[vmem] * 5,
            out_specs=[hbm] * 7,
            scratch_shapes=[pltpu.SemaphoreType.DMA((7,))],
            compiler_params=pltpu.CompilerParams(vmem_limit_bytes=1024 * 1024),
            name="store",
        )(*[pltpu.with_memory_space_constraint(x, pltpu.VMEM) for x in (og, ou, od, sc, ro)])
        fr = fr.reshape(owners * rw.shape[1], rows * LANES)
        return (jnp.swapaxes(fg, 1, 2), jnp.swapaxes(fu, 1, 2), fd, a, b, c, fr.T)

    placed = (
        P("owner", "rows", None),
        P("owner", "rows", None),
        P("owner", "rows", None),
        P("owner", "rows", None),
        P("owner", None, "rows"),
        P("owner", None, "rows"),
        P("rows", "owner"),
        P("rows"),
    )
    return jax.shard_map(
        body,
        mesh=mesh,
        in_specs=placed,
        out_specs=(
            P("owner", None, "rows"),
            P("owner", None, "rows"),
            P("owner", "rows", None),
            P("owner", "rows"),
            P("owner", "rows"),
            P("owner", "rows"),
            P(),
        ),
        check_vma=False,
    )
```

```python
import functools

import jax
import jax.numpy as jnp
from jax import lax
from jax.experimental import pallas as pl
from jax.experimental.pallas import tpu as pltpu
from jax.sharding import PartitionSpec as P

F32 = jnp.float32
BF16 = jnp.bfloat16
MESH = pl.DeviceIdType.MESH
Y = 4
LANES = 128


FIRST = 2
CORES = 2


def exchange_kernel(
    rows,
    owners,
    mg, sg, mu, su, md, sd, rw, gain,
    og, ou, od, sc, ro,
    vmg, vsg, vmu, vsu, vmd, vsd, vrw, vgain,
    send, early, tot, part_b, part_c, got_b, got_c, sum_b, sum_c,
    in_sem, small_sem, stat_send, stat_recv,
    data_send, data_recv, row_send, row_recv, own_send, own_recv, half_send, half_recv,
):
    experts = mg.shape[0]
    width = mg.shape[2]
    blocks = width // LANES
    mine = width // rows
    halves = rows // blocks
    share = LANES // mine
    owner = lax.axis_index("owner")
    me = lax.axis_index("rows")
    z, y = me // Y, me % Y
    peers = [((z + k // Y) % (rows // Y)) * Y + (y + k % Y) % Y for k in range(1, rows)]
    core = owner % CORES
    others = [(owner + k) % owners for k in range(CORES, owners, CORES)]
    partner = owner + 1 - 2 * core
    lanes = pl.ds(pl.multiple_of(me * LANES, LANES), LANES)

    barrier = pltpu.get_barrier_semaphore()
    for p in peers:
        pl.semaphore_signal(barrier, inc=1, device_id={"rows": p}, device_id_type=MESH)
    for p in others:
        pl.semaphore_signal(barrier, inc=1, device_id={"owner": p}, device_id_type=MESH)

    @pl.when(core == 0)
    def _():
        pl.semaphore_signal(barrier, inc=1, device_id={"owner": partner}, device_id_type=MESH)

    matrices = (
        (mg, sg, vmg, vsg, og, True),
        (mu, su, vmu, vsu, ou, True),
        (md, sd, vmd, vsd, od, False),
    )

    def loads(m, e):
        master, second, vm, vs = matrices[m][:4]
        return (
            pltpu.make_async_copy(master.at[e], vm.at[e], in_sem.at[2 * m, e]),
            pltpu.make_async_copy(second.at[e], vs.at[e], in_sem.at[2 * m + 1, e]),
        )

    small = (
        pltpu.make_async_copy(rw, vrw, small_sem.at[0]),
        pltpu.make_async_copy(gain, vgain, small_sem.at[1]),
    )
    for m in range(3):
        @pl.loop(0, experts)
        def _(e):
            for c in loads(m, e):
                c.start()
    for c in small:
        c.start()

    def block(b):
        return slice(b * LANES, (b + 1) * LANES)

    def partial_sums(m, e):
        vm, vs, across = matrices[m][2], matrices[m][3], matrices[m][5]
        for c in loads(m, e):
            c.wait()
        if across:
            acc = jnp.zeros((8, width), F32)
            for i in range(0, vm.shape[1], 16):
                x = vm[e, i : i + 16, :] + vs[e, i : i + 16, :].astype(F32)
                x = x * x
                acc = acc + x[:8] + x[8:]
            total = jnp.sum(acc, axis=0, keepdims=True)
            return [total[:, block(b)] for b in range(blocks)]
        result = []
        for b in range(blocks):
            x = vm[e, block(b), :] + vs[e, block(b), :].astype(F32)
            result.append(jnp.sum((x * x).T, axis=0, keepdims=True))
        return result

    def ship(m, e, totals):
        vm, vs, out, across = matrices[m][2], matrices[m][3], matrices[m][4], matrices[m][5]
        for j in range(blocks):
            b = (me // share + j) % blocks
            at = pl.ds(pl.multiple_of(b * LANES, LANES), LANES)
            inverse = 1.0 / jnp.sqrt(totals(b))
            if across:
                x = (vm[e, :, at] + vs[e, :, at].astype(F32)) * inverse
                send[m, e, at, :] = x.T.astype(BF16)
            else:
                x = vm[e, at, :] + vs[e, at, :].astype(F32)
                send[m, e, at, :] = (x * jnp.broadcast_to(inverse, (LANES, LANES)).T).astype(BF16)
            for k in range(share) if j else range(1, share):
                p = b * share + (me + k) % share
                pltpu.make_async_remote_copy(
                    src_ref=send.at[m, e, pl.ds(pl.multiple_of(p * mine, mine), mine)],
                    dst_ref=out.at[e, :, lanes],
                    send_sem=data_send.at[m], recv_sem=data_recv.at[m],
                    device_id={"rows": p}, device_id_type=MESH,
                ).start()
        out[e, :, lanes] = send[m, e, pl.ds(pl.multiple_of(me * mine, mine), mine), :]

    def to_peers(src, dst, at):
        for p in peers:
            pltpu.make_async_remote_copy(
                src_ref=src(p), dst_ref=dst, send_sem=stat_send.at[at], recv_sem=stat_recv.at[at],
                device_id={"rows": p}, device_id_type=MESH,
            ).start()

    def arrived(ref, sem):
        shares = ref.at[pl.ds(0, rows - 1)]
        pltpu.make_async_copy(shares, shares, sem).wait()

    @pl.loop(0, FIRST)
    def _(e):
        for b, row in enumerate(partial_sums(0, e)):
            early[me, e, b : b + 1, :] = row

    pl.semaphore_wait(barrier, rows - 1 + len(others) + core)
    to_peers(lambda p: early.at[me], early.at[me], 0)

    @pl.loop(FIRST, experts)
    def _(e):
        for b, row in enumerate(partial_sums(0, e)):
            part_b[(e - FIRST) % halves, b, (e - FIRST) // halves] = row

    to_peers(lambda p: part_b.at[p // blocks, p % blocks], got_b.at[me], 1)
    got_b[me] = part_b[me // blocks, me % blocks]

    for c in small:
        c.wait()
    ro[core, owner // CORES, :, lanes] = (vrw[...] * vgain[...]).astype(BF16)
    for p in peers:
        pltpu.make_async_remote_copy(
            src_ref=ro.at[core, owner // CORES, :, lanes], dst_ref=ro.at[core, owner // CORES, :, lanes],
            send_sem=row_send, recv_sem=row_recv, device_id={"rows": p}, device_id_type=MESH,
        ).start()

    @pl.loop(0, experts)
    def _(e):
        for b, row in enumerate(partial_sums(1, e)):
            part_c[e % halves, b, e // halves] = row

    arrived(early, stat_recv.at[0])
    total = early[0]
    for k in range(1, rows):
        total = total + early[k]
    tot[...] = total

    def early_totals(e):
        return lambda b: tot[e, pl.ds(b, 1), :]

    def stage_totals(ref, at):
        return lambda b: ref[(at % halves) * blocks + b, at // halves]

    ship(0, 0, early_totals(0))

    def add_up(got, whole, at):
        arrived(got, stat_recv.at[at])
        total = got[0]
        for k in range(1, rows):
            total = total + got[k]
        whole[me] = total
        to_peers(lambda p: whole.at[me], whole.at[me], at + 1)

    add_up(got_b, sum_b, 1)

    @pl.loop(1, FIRST)
    def _(e):
        ship(0, e, early_totals(e))

    @pl.loop(0, experts)
    def _(e):
        for b, row in enumerate(partial_sums(2, e)):
            part_c[e % halves, b, (experts + e) // halves] = row

    to_peers(lambda p: part_c.at[p // blocks, p % blocks], got_c.at[me], 3)
    got_c[me] = part_c[me // blocks, me % blocks]

    arrived(sum_b, stat_recv.at[2])

    def ship_gate(e):
        ship(0, e, stage_totals(sum_b, e - FIRST))

    pl.loop(FIRST, experts - 2)(ship_gate)
    add_up(got_c, sum_c, 3)
    pl.loop(experts - 2, experts)(ship_gate)

    row = ro.at[core, owner // CORES, :, pl.ds(0, (rows - 1) * LANES)]
    pltpu.make_async_copy(row, row, row_recv).wait()
    pltpu.make_async_copy(row, row, row_send).wait()
    for p in others:
        pltpu.make_async_remote_copy(
            src_ref=ro.at[core, owner // CORES], dst_ref=ro.at[core, owner // CORES],
            send_sem=own_send, recv_sem=own_recv, device_id={"owner": p}, device_id_type=MESH,
        ).start()

    def ship_rest(m):
        @pl.loop(0, experts)
        def _(e):
            ship(m, e, stage_totals(sum_c, (m - 1) * experts + e))

    arrived(sum_c, stat_recv.at[4])
    ship_rest(1)

    theirs = ro.at[core, pl.ds(0, owners // CORES - 1)]
    pltpu.make_async_copy(theirs, theirs, own_send).wait()
    pltpu.make_async_copy(theirs, theirs, own_recv).wait()
    half = pltpu.make_async_remote_copy(
        src_ref=ro.at[core], dst_ref=ro.at[core],
        send_sem=half_send, recv_sem=half_recv, device_id={"owner": partner}, device_id_type=MESH,
    )

    @pl.when(core == 1)
    def _():
        half.start()

    @pl.when(core == 0)
    def _():
        half.wait_recv()
        half.start()

    ship_rest(2)

    def own_scale(value):
        value = jnp.sqrt(value)
        value = jnp.where(me % 2 == 1, pltpu.roll(value, LANES - mine, 1), value)
        return value[:, :mine]

    pair = me // 2
    for e in range(FIRST):
        sc[0, e : e + 1, :] = own_scale(tot[e, pl.ds(pair, 1), :])
    for u in range(3 * experts - FIRST):
        m, e = (u + FIRST) // experts, (u + FIRST) % experts
        ref, at = (sum_b, u) if m == 0 else (sum_c, u + FIRST - experts)
        sc[m, e : e + 1, :] = own_scale(ref[(at % halves) * blocks + pair, at // halves])

    for at, ref in enumerate((early, got_b, sum_b, got_c, sum_c)):
        arrived(ref, stat_send.at[at])
    half.wait_send()

    @pl.when(core == 1)
    def _():
        half.wait_recv()

    for m in range(3):
        sent = send.at[m, :, pl.ds(0, (rows - 1) * mine), :]
        pltpu.make_async_copy(sent, sent, data_send.at[m]).wait()
        pltpu.make_async_copy(sent, sent, data_recv.at[m]).wait()


def store_kernel(og, ou, od, sc, ro, fg, fu, fd, a, b, c, fr, sem):
    copies = [
        pltpu.make_async_copy(og, fg, sem.at[0]),
        pltpu.make_async_copy(ou, fu, sem.at[1]),
        pltpu.make_async_copy(od, fd, sem.at[2]),
        pltpu.make_async_copy(ro.at[0], fr.at[:, 0], sem.at[3]),
        pltpu.make_async_copy(ro.at[1], fr.at[:, 1], sem.at[7]),
        pltpu.make_async_copy(sc.at[0], a, sem.at[4]),
        pltpu.make_async_copy(sc.at[1], b, sem.at[5]),
        pltpu.make_async_copy(sc.at[2], c, sem.at[6]),
    ]
    for copy in copies:
        copy.start()
    for copy in copies:
        copy.wait()


def solution(mesh):
    owners, rows = mesh.shape["owner"], mesh.shape["rows"]

    def body(mg, sg, mu, su, md, sd, rw, gain):
        experts, deep, width = mg.shape
        blocks = width // LANES
        halves = rows // blocks
        units_b = (experts - FIRST) // halves
        units_c = 2 * experts // halves
        mine = width // rows
        hbm = pl.BlockSpec(memory_space=pltpu.HBM)
        vmem = pl.BlockSpec(memory_space=pltpu.VMEM)
        result = pltpu.VMEM((experts, mine, rows * LANES), BF16)
        args = [mg, sg, mu, su, md, sd, rw.T, gain[None, :]]
        args = [pltpu.with_memory_space_constraint(x, pltpu.HBM) for x in args]
        og, ou, od, sc, ro = pl.pallas_call(
            functools.partial(exchange_kernel, rows, owners),
            out_shape=[
                result, result, result,
                pltpu.VMEM((3, experts, mine), F32),
                pltpu.VMEM((CORES, owners // CORES, rw.shape[1], rows * LANES), BF16),
            ],
            in_specs=[hbm] * 8,
            out_specs=[vmem] * 5,
            scratch_shapes=[pltpu.VMEM(x.shape, x.dtype) for x in args]
            + [
                pltpu.VMEM((3, experts, width, LANES), BF16),
                pltpu.VMEM((rows, FIRST, blocks, LANES), F32),
                pltpu.VMEM((FIRST, blocks, LANES), F32),
                pltpu.VMEM((halves, blocks, units_b, 1, LANES), F32),
                pltpu.VMEM((halves, blocks, units_c, 1, LANES), F32),
                pltpu.VMEM((rows, units_b, 1, LANES), F32),
                pltpu.VMEM((rows, units_c, 1, LANES), F32),
                pltpu.VMEM((rows, units_b, 1, LANES), F32),
                pltpu.VMEM((rows, units_c, 1, LANES), F32),
                pltpu.SemaphoreType.DMA((6, experts)),
                pltpu.SemaphoreType.DMA((2,)),
                pltpu.SemaphoreType.DMA((5,)),
                pltpu.SemaphoreType.DMA((5,)),
                pltpu.SemaphoreType.DMA((3,)),
                pltpu.SemaphoreType.DMA((3,)),
                pltpu.SemaphoreType.DMA,
                pltpu.SemaphoreType.DMA,
                pltpu.SemaphoreType.DMA,
                pltpu.SemaphoreType.DMA,
                pltpu.SemaphoreType.DMA,
                pltpu.SemaphoreType.DMA,
            ],
            compiler_params=pltpu.CompilerParams(
                collective_id=0, has_side_effects=True, vmem_limit_bytes=44 * 1024 * 1024
            ),
            name="exchange",
        )(*args)
        scale = jax.ShapeDtypeStruct((experts, mine), F32)
        whole = jax.ShapeDtypeStruct((experts, mine, rows * LANES), BF16)
        fg, fu, fd, a, b, c, fr = pl.pallas_call(
            store_kernel,
            out_shape=[whole] * 3 + [scale] * 3 + [jax.ShapeDtypeStruct((owners // CORES, CORES, *ro.shape[2:]), BF16)],
            in_specs=[vmem] * 5,
            out_specs=[hbm] * 7,
            scratch_shapes=[pltpu.SemaphoreType.DMA((8,))],
            compiler_params=pltpu.CompilerParams(vmem_limit_bytes=1024 * 1024),
            name="store",
        )(*[pltpu.with_memory_space_constraint(x, pltpu.VMEM) for x in (og, ou, od, sc, ro)])
        fr = fr.reshape(owners * rw.shape[1], rows * LANES)
        return (jnp.swapaxes(fg, 1, 2), jnp.swapaxes(fu, 1, 2), fd, a, b, c, fr.T)

    placed = (
        P("owner", "rows", None),
        P("owner", "rows", None),
        P("owner", "rows", None),
        P("owner", "rows", None),
        P("owner", None, "rows"),
        P("owner", None, "rows"),
        P("rows", "owner"),
        P("rows"),
    )
    return jax.shard_map(
        body,
        mesh=mesh,
        in_specs=placed,
        out_specs=(
            P("owner", None, "rows"),
            P("owner", None, "rows"),
            P("owner", "rows", None),
            P("owner", "rows"),
            P("owner", "rows"),
            P("owner", "rows"),
            P(),
        ),
        check_vma=False,
    )
```

```python
import functools

import jax
import jax.numpy as jnp
from jax import lax
from jax.experimental import pallas as pl
from jax.experimental.pallas import tpu as pltpu
from jax.sharding import PartitionSpec as P

F32 = jnp.float32
BF16 = jnp.bfloat16
MESH = pl.DeviceIdType.MESH
Y = 4
LANES = 128


FIRST = 2
PLAIN = 32
CORES = 2


def exchange_kernel(
    rows,
    owners,
    mg, sg, mu, su, md, sd, rw, gain,
    og, ou, od, sc, ro,
    vmg, vsg, vmu, vsu, vmd, vsd, vrw, vgain,
    send, plain, landed, spread, early, tot, part_b, part_c, got_b, got_c, sum_b, sum_c,
    in_sem, small_sem, stat_send, stat_recv,
    data_send, data_recv, plain_send, plain_recv, row_send, row_recv, own_send, own_recv, half_send, half_recv,
):
    experts = mg.shape[0]
    width = mg.shape[2]
    blocks = width // LANES
    mine = width // rows
    halves = rows // blocks
    share = LANES // mine
    owner = lax.axis_index("owner")
    me = lax.axis_index("rows")
    z, y = me // Y, me % Y
    peers = [((z + k // Y) % (rows // Y)) * Y + (y + k % Y) % Y for k in range(1, rows)]
    core = owner % CORES
    others = [(owner + k) % owners for k in range(CORES, owners, CORES)]
    partner = owner + 1 - 2 * core
    lanes = pl.ds(pl.multiple_of(me * LANES, LANES), LANES)

    barrier = pltpu.get_barrier_semaphore()
    for p in peers:
        pl.semaphore_signal(barrier, inc=1, device_id={"rows": p}, device_id_type=MESH)
    for p in others:
        pl.semaphore_signal(barrier, inc=1, device_id={"owner": p}, device_id_type=MESH)

    @pl.when(core == 0)
    def _():
        pl.semaphore_signal(barrier, inc=1, device_id={"owner": partner}, device_id_type=MESH)

    matrices = (
        (mg, sg, vmg, vsg, og, True),
        (mu, su, vmu, vsu, ou, True),
        (md, sd, vmd, vsd, od, False),
    )

    def loads(m, e):
        master, second, vm, vs = matrices[m][:4]
        return (
            pltpu.make_async_copy(master.at[e], vm.at[e], in_sem.at[2 * m, e]),
            pltpu.make_async_copy(second.at[e], vs.at[e], in_sem.at[2 * m + 1, e]),
        )

    small = (
        pltpu.make_async_copy(rw, vrw, small_sem.at[0]),
        pltpu.make_async_copy(gain, vgain, small_sem.at[1]),
    )

    def start_loads(m, lo, hi):
        @pl.loop(lo, hi)
        def _(e):
            for c in loads(m, e):
                c.start()

    start_loads(0, 0, FIRST)
    start_loads(2, experts - 1, experts)
    start_loads(0, FIRST, experts)
    for c in small:
        c.start()

    def block(b):
        return slice(b * LANES, (b + 1) * LANES)

    def partial_sums(m, e, wait=True):
        vm, vs, across = matrices[m][2], matrices[m][3], matrices[m][5]
        for c in loads(m, e) if wait else ():
            c.wait()
        if across:
            acc = jnp.zeros((8, width), F32)
            for i in range(0, vm.shape[1], 16):
                x = vm[e, i : i + 16, :] + vs[e, i : i + 16, :].astype(F32)
                x = x * x
                acc = acc + x[:8] + x[8:]
            total = jnp.sum(acc, axis=0, keepdims=True)
            return [total[:, block(b)] for b in range(blocks)]
        result = []
        for b in range(blocks):
            x = vm[e, block(b), :] + vs[e, block(b), :].astype(F32)
            result.append(jnp.sum((x * x).T, axis=0, keepdims=True))
        return result

    last = experts - 1

    def ship(m, e, totals, skip=0):
        vm, vs, out, across = matrices[m][2], matrices[m][3], matrices[m][4], matrices[m][5]
        for j in range(blocks):
            b = (me // share + j) % blocks
            at = pl.ds(pl.multiple_of(b * LANES, LANES), LANES)
            inverse = 1.0 / jnp.sqrt(totals(b))
            if across:
                x = (vm[e, :, at] + vs[e, :, at].astype(F32)) * inverse
                send[m, e, at, :] = x.T.astype(BF16)
            else:
                x = vm[e, at, :] + vs[e, at, :].astype(F32)
                send[m, e, at, :] = (x * jnp.broadcast_to(inverse, (LANES, LANES)).T).astype(BF16)
            for k in range(share) if j else range(1, share):
                p = b * share + (me + k) % share
                pltpu.make_async_remote_copy(
                    src_ref=send.at[m, e, pl.ds(pl.multiple_of(p * mine + skip, 16), mine - skip)],
                    dst_ref=out.at[e, skip:, lanes],
                    send_sem=data_send.at[m + (skip > 0)], recv_sem=data_recv.at[m + (skip > 0)],
                    device_id={"rows": p}, device_id_type=MESH,
                ).start()
        out[e, skip:, lanes] = send[m, e, pl.ds(pl.multiple_of(me * mine + skip, 16), mine - skip), :]

    def to_peers(src, dst, at):
        for p in peers:
            pltpu.make_async_remote_copy(
                src_ref=src(p), dst_ref=dst, send_sem=stat_send.at[at], recv_sem=stat_recv.at[at],
                device_id={"rows": p}, device_id_type=MESH,
            ).start()

    def arrived(ref, sem):
        shares = ref.at[pl.ds(0, rows - 1)]
        pltpu.make_async_copy(shares, shares, sem).wait()

    @pl.loop(0, FIRST)
    def _(e):
        for b, row in enumerate(partial_sums(0, e)):
            early[me, e, b : b + 1, :] = row

    pl.semaphore_wait(barrier, rows - 1 + len(others) + core)
    to_peers(lambda p: early.at[me], early.at[me], 0)

    @pl.loop(FIRST, experts)
    def _(e):
        for b, row in enumerate(partial_sums(0, e)):
            part_b[(e - FIRST) % halves, b, (e - FIRST) // halves] = row

    to_peers(lambda p: part_b.at[p // blocks, p % blocks], got_b.at[me], 1)
    got_b[me] = part_b[me // blocks, me % blocks]

    for c in loads(2, last):
        c.wait()

    @pl.loop(0, rows)
    def _(p):
        at = pl.ds(pl.multiple_of(p * mine, mine), PLAIN)
        plain[p] = vmd[last, at, :] + vsd[last, at, :].astype(F32)

    for p in peers:
        pltpu.make_async_remote_copy(
            src_ref=plain.at[p], dst_ref=landed.at[me], send_sem=plain_send, recv_sem=plain_recv,
            device_id={"rows": p}, device_id_type=MESH,
        ).start()
    landed[me] = plain[me]
    start_loads(1, 0, experts)

    arrived(early, stat_recv.at[0])
    total = early[0]
    for k in range(1, rows):
        total = total + early[k]
    tot[...] = total

    def early_totals(e):
        return lambda b: tot[e, pl.ds(b, 1), :]

    def stage_totals(ref, at):
        return lambda b: ref[(at % halves) * blocks + b, at // halves]

    ship(0, 0, early_totals(0))

    for c in small:
        c.wait()
    ro[core, owner // CORES, :, lanes] = (vrw[...] * vgain[...]).astype(BF16)
    for p in peers:
        pltpu.make_async_remote_copy(
            src_ref=ro.at[core, owner // CORES, :, lanes], dst_ref=ro.at[core, owner // CORES, :, lanes],
            send_sem=row_send, recv_sem=row_recv, device_id={"rows": p}, device_id_type=MESH,
        ).start()

    def add_up(got, whole, at):
        arrived(got, stat_recv.at[at])
        total = got[0]
        for k in range(1, rows):
            total = total + got[k]
        whole[me] = total
        to_peers(lambda p: whole.at[me], whole.at[me], at + 1)

    add_up(got_b, sum_b, 1)

    @pl.loop(1, FIRST)
    def _(e):
        ship(0, e, early_totals(e))

    start_loads(2, 0, last)

    @pl.loop(0, experts)
    def _(e):
        for b, row in enumerate(partial_sums(1, e)):
            part_c[e % halves, b, e // halves] = row

    @pl.loop(0, last)
    def _(e):
        for b, row in enumerate(partial_sums(2, e)):
            part_c[e % halves, b, (experts + e) // halves] = row

    for b, row in enumerate(partial_sums(2, last, False)):
        part_c[last % halves, b, (experts + last) // halves] = row

    to_peers(lambda p: part_c.at[p // blocks, p % blocks], got_c.at[me], 3)
    got_c[me] = part_c[me // blocks, me % blocks]

    arrived(sum_b, stat_recv.at[2])

    def ship_gate(e):
        ship(0, e, stage_totals(sum_b, e - FIRST))

    pl.loop(FIRST, experts - 2)(ship_gate)
    add_up(got_c, sum_c, 3)
    pl.loop(experts - 2, experts)(ship_gate)

    row = ro.at[core, owner // CORES, :, pl.ds(0, (rows - 1) * LANES)]
    pltpu.make_async_copy(row, row, row_recv).wait()
    pltpu.make_async_copy(row, row, row_send).wait()
    for p in others:
        pltpu.make_async_remote_copy(
            src_ref=ro.at[core, owner // CORES], dst_ref=ro.at[core, owner // CORES],
            send_sem=own_send, recv_sem=own_recv, device_id={"owner": p}, device_id_type=MESH,
        ).start()

    def ship_rest(m, lo, hi, skip=0):
        pl.loop(lo, hi)(lambda e: ship(m, e, stage_totals(sum_c, (m - 1) * experts + e), skip))

    arrived(sum_c, stat_recv.at[4])
    ship_rest(1, 0, experts)

    theirs = ro.at[core, pl.ds(0, owners // CORES - 1)]
    pltpu.make_async_copy(theirs, theirs, own_send).wait()
    pltpu.make_async_copy(theirs, theirs, own_recv).wait()
    half = pltpu.make_async_remote_copy(
        src_ref=ro.at[core], dst_ref=ro.at[core],
        send_sem=half_send, recv_sem=half_recv, device_id={"owner": partner}, device_id_type=MESH,
    )

    @pl.when(core == 1)
    def _():
        half.start()

    @pl.when(core == 0)
    def _():
        half.wait_recv()
        half.start()

    ship_rest(2, 0, last)
    ship_rest(2, last, experts, PLAIN)

    inverse = 1.0 / jnp.sqrt(stage_totals(sum_c, experts + last)(me // share))
    spread[...] = jnp.broadcast_to(inverse, (LANES, LANES)).T
    scale = spread[pl.ds(pl.multiple_of((me % share) * mine, mine), PLAIN), :]
    arrived(landed, plain_recv)
    for k in range(rows):
        od[last, :PLAIN, k * LANES : (k + 1) * LANES] = (landed[k] * scale).astype(BF16)

    def own_scale(value):
        value = jnp.sqrt(value)
        value = jnp.where(me % 2 == 1, pltpu.roll(value, LANES - mine, 1), value)
        return value[:, :mine]

    pair = me // 2
    for e in range(FIRST):
        sc[0, e : e + 1, :] = own_scale(tot[e, pl.ds(pair, 1), :])
    for u in range(3 * experts - FIRST):
        m, e = (u + FIRST) // experts, (u + FIRST) % experts
        ref, at = (sum_b, u) if m == 0 else (sum_c, u + FIRST - experts)
        sc[m, e : e + 1, :] = own_scale(ref[(at % halves) * blocks + pair, at // halves])

    for at, ref in enumerate((early, got_b, sum_b, got_c, sum_c)):
        arrived(ref, stat_send.at[at])
    half.wait_send()

    @pl.when(core == 1)
    def _():
        half.wait_recv()

    arrived(landed, plain_send)
    for m in range(4):
        if m < 2:
            sent = send.at[m, :, pl.ds(0, (rows - 1) * mine), :]
        elif m == 2:
            sent = send.at[m, pl.ds(0, last), pl.ds(0, (rows - 1) * mine), :]
        else:
            sent = send.at[2, last, pl.ds(0, (rows - 1) * (mine - PLAIN)), :]
        pltpu.make_async_copy(sent, sent, data_send.at[m]).wait()
        pltpu.make_async_copy(sent, sent, data_recv.at[m]).wait()


def store_kernel(og, ou, od, sc, ro, fg, fu, fd, a, b, c, fr, sem):
    copies = [
        pltpu.make_async_copy(og, fg, sem.at[0]),
        pltpu.make_async_copy(ou, fu, sem.at[1]),
        pltpu.make_async_copy(od, fd, sem.at[2]),
        pltpu.make_async_copy(ro.at[0], fr.at[:, 0], sem.at[3]),
        pltpu.make_async_copy(ro.at[1], fr.at[:, 1], sem.at[7]),
        pltpu.make_async_copy(sc.at[0], a, sem.at[4]),
        pltpu.make_async_copy(sc.at[1], b, sem.at[5]),
        pltpu.make_async_copy(sc.at[2], c, sem.at[6]),
    ]
    for copy in copies:
        copy.start()
    for copy in copies:
        copy.wait()


def solution(mesh):
    owners, rows = mesh.shape["owner"], mesh.shape["rows"]

    def body(mg, sg, mu, su, md, sd, rw, gain):
        experts, deep, width = mg.shape
        blocks = width // LANES
        halves = rows // blocks
        units_b = (experts - FIRST) // halves
        units_c = 2 * experts // halves
        mine = width // rows
        hbm = pl.BlockSpec(memory_space=pltpu.HBM)
        vmem = pl.BlockSpec(memory_space=pltpu.VMEM)
        result = pltpu.VMEM((experts, mine, rows * LANES), BF16)
        args = [mg, sg, mu, su, md, sd, rw.T, gain[None, :]]
        args = [pltpu.with_memory_space_constraint(x, pltpu.HBM) for x in args]
        og, ou, od, sc, ro = pl.pallas_call(
            functools.partial(exchange_kernel, rows, owners),
            out_shape=[
                result, result, result,
                pltpu.VMEM((3, experts, mine), F32),
                pltpu.VMEM((CORES, owners // CORES, rw.shape[1], rows * LANES), BF16),
            ],
            in_specs=[hbm] * 8,
            out_specs=[vmem] * 5,
            scratch_shapes=[pltpu.VMEM(x.shape, x.dtype) for x in args]
            + [
                pltpu.VMEM((3, experts, width, LANES), BF16),
                pltpu.VMEM((rows, PLAIN, LANES), F32),
                pltpu.VMEM((rows, PLAIN, LANES), F32),
                pltpu.VMEM((LANES, LANES), F32),
                pltpu.VMEM((rows, FIRST, blocks, LANES), F32),
                pltpu.VMEM((FIRST, blocks, LANES), F32),
                pltpu.VMEM((halves, blocks, units_b, 1, LANES), F32),
                pltpu.VMEM((halves, blocks, units_c, 1, LANES), F32),
                pltpu.VMEM((rows, units_b, 1, LANES), F32),
                pltpu.VMEM((rows, units_c, 1, LANES), F32),
                pltpu.VMEM((rows, units_b, 1, LANES), F32),
                pltpu.VMEM((rows, units_c, 1, LANES), F32),
                pltpu.SemaphoreType.DMA((6, experts)),
                pltpu.SemaphoreType.DMA((2,)),
                pltpu.SemaphoreType.DMA((5,)),
                pltpu.SemaphoreType.DMA((5,)),
                pltpu.SemaphoreType.DMA((4,)),
                pltpu.SemaphoreType.DMA((4,)),
                pltpu.SemaphoreType.DMA,
                pltpu.SemaphoreType.DMA,
                pltpu.SemaphoreType.DMA,
                pltpu.SemaphoreType.DMA,
                pltpu.SemaphoreType.DMA,
                pltpu.SemaphoreType.DMA,
                pltpu.SemaphoreType.DMA,
                pltpu.SemaphoreType.DMA,
            ],
            compiler_params=pltpu.CompilerParams(
                collective_id=0, has_side_effects=True, vmem_limit_bytes=44 * 1024 * 1024
            ),
            name="exchange",
        )(*args)
        scale = jax.ShapeDtypeStruct((experts, mine), F32)
        whole = jax.ShapeDtypeStruct((experts, mine, rows * LANES), BF16)
        fg, fu, fd, a, b, c, fr = pl.pallas_call(
            store_kernel,
            out_shape=[whole] * 3 + [scale] * 3 + [jax.ShapeDtypeStruct((owners // CORES, CORES, *ro.shape[2:]), BF16)],
            in_specs=[vmem] * 5,
            out_specs=[hbm] * 7,
            scratch_shapes=[pltpu.SemaphoreType.DMA((8,))],
            compiler_params=pltpu.CompilerParams(vmem_limit_bytes=1024 * 1024),
            name="store",
        )(*[pltpu.with_memory_space_constraint(x, pltpu.VMEM) for x in (og, ou, od, sc, ro)])
        fr = fr.reshape(owners * rw.shape[1], rows * LANES)
        return (jnp.swapaxes(fg, 1, 2), jnp.swapaxes(fu, 1, 2), fd, a, b, c, fr.T)

    placed = (
        P("owner", "rows", None),
        P("owner", "rows", None),
        P("owner", "rows", None),
        P("owner", "rows", None),
        P("owner", None, "rows"),
        P("owner", None, "rows"),
        P("rows", "owner"),
        P("rows"),
    )
    return jax.shard_map(
        body,
        mesh=mesh,
        in_specs=placed,
        out_specs=(
            P("owner", None, "rows"),
            P("owner", None, "rows"),
            P("owner", "rows", None),
            P("owner", "rows"),
            P("owner", "rows"),
            P("owner", "rows"),
            P(),
        ),
        check_vma=False,
    )
```
